32 devices in a mesh: groups: 2 (over y), tm: 4 (over z), chan: 4 (over x, core).
Axes of the slice: x: 2, y: 2, z: 4, core: 2. Of those that a mesh axis runs over, the one named last changes fastest.
Arguments:
- vis: bfloat16 [8, 128, 2, 128], P(('groups', 'chan'), 'tm'), parts along dimension 0, may hold values from -6 to 6
- row_weight: bfloat16 [8, 128, 128, 128], P(('groups', 'chan'), 'tm'), parts along dimension 0, may hold values from -4 to 4
- col_weight: bfloat16 [8, 128, 128, 256], P(('groups', 'chan'), 'tm'), parts along dimension 0, may hold values from -0.5 to 0.5
- w_bin: int32 [8, 128, 1], P(('groups', 'chan'), 'tm'), parts along dimension 0, may hold values from 0 to 3; in each aligned block of 32 rows (0 to 31, 32 to 63, ..., all dimensions but the last counted through in order) at most 16 rows name the same one
- tile_col: int32 [8, 128], P(('groups', 'chan'), 'tm'), parts along dimension 0, may hold values from 0 to 15
- w_kernel: bfloat16 [8, 512, 512], P(('groups', 'tm')), parts along dimension 0, may hold values from -0.25 to 0.25
Outputs:
- grid: float32 [8, 128, 16, 512], P(('groups', 'tm'), 'chan'), parts along dimension 0
The draws below stay inside these ranges and needn't reach their ends.
There are 2 independent parts, one for each index of `groups`. The reference program is written for one: setup_inputs(seed, part) draws one part's arguments, and reference() takes and returns one part's arrays. A program takes and returns all parts, laid end to end along the dimension named above; each array names one. Nothing has to cross between parts.
Inputs may be any that keep to these rules, and one draw needn't show every extreme that they name: `w_bin`: within the blocks of one device (aligned blocks of 32 along the channel-group and block dimensions taken together), no w-plane is named more than 16 times, a bound that some block reaches.
All inputs are finite; a program needn't handle non-finite values.
Results may differ from the reference program's by a relative error of at most 0.0041.
Values may be sent and summed in bfloat16 or wider, within the bound.
A program may use at most 128 MiB of HBM per device.

```python
import math
import jax
import jax.numpy as jnp
import numpy as np
from jax import lax

VIS = 128
KROWS = 128
QW = 256
BLK_DEV = 32
TC = 16
NW = 4
BLOCKS = 128
CHANS = 4
CAP = 16


def touch_ends(drawn, stream_key, smallest, top_value):
    spot = [jax.random.randint(jax.random.fold_in(stream_key, axis), (), 0, length) for axis, length in enumerate(drawn.shape)]
    longest = drawn.shape.index(max(drawn.shape))
    next_to = spot[:longest] + [(spot[longest] + 1) % drawn.shape[longest]] + spot[longest + 1:]
    return drawn.at[tuple(spot)].set(smallest).at[tuple(next_to)].set(top_value)


def steps_of(own_key, extent, cuts, low, high):
    def one(dim, blocks):
        steps = jax.random.uniform(jax.random.fold_in(jax.random.fold_in(own_key, 6), dim), (blocks,), jnp.float32, low / len(cuts), high / len(cuts))
        return jnp.repeat(jnp.exp(steps), extent[dim] // blocks).reshape((-1,) + (1,) * (len(extent) - dim - 1))

    level = one(*cuts[0])
    for cut in cuts[1:]:
        level = level * one(*cut)
    return level


def deal_out(rng, own, number, rows, count, top, most, skew):
    ranking = jax.random.permutation(rng, count)
    crowded, ordinary = portions_of(count, rows * top, most, skew, True), portions_of(count, rows * top, most, skew, False)
    places = jnp.arange(count)

    def named(lengths, turn):
        used = int((lengths > 0).sum())
        fixed = max(1, used // 4)
        moved = fixed + (places - fixed + turn * (used - fixed)) % max(1, count - fixed)
        return jnp.zeros((count,), jnp.int32).at[ranking[jnp.where(places < fixed, places, moved)]].set(jnp.asarray(lengths, jnp.int32))

    lengths = jnp.where(number % 4 == 0, named(crowded, number // 4), named(ordinary, number - number // 4 - 1))
    mixed = jax.random.permutation(jax.random.fold_in(own, 3), count)
    source_of, taker = mixed[0:count // 2 * 2:2], mixed[1:count // 2 * 2:2]
    margin = jnp.minimum(lengths[source_of] - 1, most - lengths[taker]) // 2
    margin = jnp.where((source_of == ranking[0]) | (taker == ranking[0]) | (lengths[taker] == 0), 0, jnp.maximum(margin, 0))
    moved = jax.random.randint(jax.random.fold_in(own, 4), (count // 2,), 0, 1 << 20) % (margin + 1)
    lengths = lengths.at[source_of].add(-moved).at[taker].add(moved)
    items = jnp.searchsorted(jnp.cumsum(lengths), jnp.arange(rows * top), side="right").astype(jnp.int32)
    table = items.reshape(top, rows).T
    table = table[jax.random.permutation(jax.random.fold_in(own, 1), rows)]
    turn = jax.random.randint(jax.random.fold_in(own, 2), (rows, 1), 0, top)
    return jnp.take_along_axis(table, (jnp.arange(top)[None, :] + turn) % top, axis=1)


def portions_of(number_of, total, most, skew, full):
    weights = [(1 << 20) // math.isqrt(grade ** skew) + 1 for grade in range(1, number_of + 1)]
    largest = most if full else min(most, max(-(-total // number_of), total * weights[0] // sum(weights)))
    least = 1 if total - largest >= number_of - 1 else 0
    given, spare = [largest] + [least] * (number_of - 1), total - largest - least * (number_of - 1)
    while spare > 0:
        candidates = [i for i in range(1, number_of) if given[i] < largest] or [i for i in range(1, number_of) if given[i] < most]
        whole, left = sum([weights[i] for i in candidates]), spare
        for i in candidates:
            extra = min(most - given[i], max(1, left * weights[i] // whole), spare)
            given[i] = given[i] + extra
            spare = spare - extra
    return np.array(given)


def gaussian(own_key, shape, width, reach, shards=(), held_as=jnp.bfloat16):
    loudness = steps_of(own_key, shape, shards, -0.22, 0.18) if shards else 1.0
    array = jax.random.normal(own_key, shape, jnp.float32) * width * loudness
    return jnp.minimum(jnp.maximum(array, -reach), reach).astype(held_as)


def setup_inputs(seed: int = 0, part: int = 0) -> dict:
    seeds = jax.random.split(jax.random.key(seed), 7)
    part_keys = jax.random.split(jax.random.fold_in(seeds[6], part), 7)
    vis = gaussian(part_keys[0], (CHANS, BLOCKS, 2, VIS), 1.0, 6.0, ((0, 4), (1, 4)))
    row_weight = gaussian(part_keys[1], (CHANS, BLOCKS, KROWS, VIS), 0.25, 4.0, ((0, 4), (1, 4)))
    col_weight = gaussian(part_keys[2], (CHANS, BLOCKS, VIS, QW), VIS ** -0.5, 0.5, ((0, 4), (1, 4)))
    w_bin_keys = jax.random.split(jax.random.fold_in(part_keys[3], 1), CHANS * BLOCKS // BLK_DEV)
    w_bin_turns = jax.random.permutation(jax.random.fold_in(part_keys[3], 3), CHANS * BLOCKS // BLK_DEV)
    w_bin = jax.vmap(lambda own, number: deal_out(jax.random.fold_in(part_keys[3], 2), own, number, BLK_DEV, NW, 1, CAP, 2))(w_bin_keys, w_bin_turns).reshape((CHANS, BLOCKS, 1))
    tile_col = touch_ends(jax.random.randint(part_keys[4], (CHANS, BLOCKS), 0, TC), jax.random.fold_in(part_keys[4], 1), 0, TC - 1).astype(jnp.int32)
    w_kernel = gaussian(part_keys[5], (NW, 2 * QW, 2 * QW), (2 * QW) ** -0.5, 0.25, ((0, 4),))
    return {"vis": vis, "row_weight": row_weight, "col_weight": col_weight, "w_bin": w_bin, "tile_col": tile_col, "w_kernel": w_kernel}


def reference(vis, row_weight, col_weight, w_bin, tile_col, w_kernel):
    total_blocks = CHANS * BLOCKS
    vis_all = vis.reshape(total_blocks // BLK_DEV, BLK_DEV, 2, VIS)
    rows_all = row_weight.reshape(total_blocks // BLK_DEV, BLK_DEV, KROWS, VIS)
    cols_all = col_weight.reshape(total_blocks // BLK_DEV, BLK_DEV, VIS, QW)
    seg_all = (w_bin[:, :, 0] * TC + tile_col).astype(jnp.int32).reshape(total_blocks // BLK_DEV, BLK_DEV)

    def step(acc, group):
        vis_g, rows_g, cols_g, seg_g = group
        weighted = (rows_g.astype(jnp.float32)[:, None, :, :] * vis_g.astype(jnp.float32)[:, :, None, :]).astype(jnp.bfloat16)
        patch = jnp.einsum('ghkv,gvq->gkhq', weighted.astype(jnp.float32), cols_g.astype(jnp.float32))
        patch = patch.reshape(BLK_DEV, KROWS, 2 * QW)
        return acc.at[seg_g].add(patch), None

    start = jnp.zeros((NW * TC, KROWS, 2 * QW), jnp.float32)
    acc, _ = lax.scan(step, start, (vis_all, rows_all, cols_all, seg_all))
    pre_rounded = acc.reshape(NW, TC, KROWS, 2 * QW).astype(jnp.bfloat16)
    return jnp.einsum('wtkq,wqr->wktr', pre_rounded.astype(jnp.float32), w_kernel.astype(jnp.float32))
```

```python
import functools
import jax
import jax.numpy as jnp
from jax import lax
from jax.experimental import pallas as pl
from jax.experimental.pallas import tpu as pltpu
from jax.sharding import PartitionSpec as P

QW = 256
GC = 4096
MESH = pl.DeviceIdType.MESH
LIMIT = 60 * 1024 * 1024


def pair_of(me):
    return me + 1 - 2 * (me % 2)


def swap_kernel(vis, rows, cols, seg, vis_p, rows_p, cols_p, seg_p, send, recv):
    me = lax.axis_index("chan")
    other = pair_of(me)
    barrier = pltpu.get_barrier_semaphore()
    pl.semaphore_signal(barrier, inc=1, device_id={"chan": other}, device_id_type=MESH)
    pl.semaphore_wait(barrier, 1)
    moves = ((seg, seg_p), (vis, vis_p), (rows.at[:, :, other % 2], rows_p), (cols, cols_p))
    copies = [
        pltpu.make_async_remote_copy(
            src_ref=src, dst_ref=dst, send_sem=send.at[i], recv_sem=recv.at[i],
            device_id={"chan": other}, device_id_type=MESH,
        )
        for i, (src, dst) in enumerate(moves)
    ]
    for copy in copies:
        copy.start()
    for copy in copies:
        copy.wait()


def swap(vis, rows, cols, seg):
    any_spec = pl.BlockSpec(memory_space=pl.ANY)
    count, fold, _, share, width = rows.shape
    shapes = (
        jax.ShapeDtypeStruct(vis.shape, vis.dtype),
        jax.ShapeDtypeStruct((count, fold, share, width), rows.dtype),
        jax.ShapeDtypeStruct(cols.shape, cols.dtype),
        jax.ShapeDtypeStruct(seg.shape, seg.dtype),
    )
    return pl.pallas_call(
        swap_kernel,
        out_shape=shapes,
        in_specs=[any_spec] * 4,
        out_specs=[any_spec] * 4,
        scratch_shapes=[pltpu.SemaphoreType.DMA((4,)), pltpu.SemaphoreType.DMA((4,))],
        compiler_params=pltpu.CompilerParams(collective_id=0, has_side_effects=True),
        name="swap",
    )(vis, rows, cols, seg)


def patch_kernel(cells, batch, seg_o, seg_p, half, vis_o, rows_o, cols_o, vis_p, rows_p, cols_p, out, acc):
    g, s = pl.program_id(0), pl.program_id(1)
    fold, share = out.shape[0], out.shape[2]
    span = fold * share

    @pl.when(s == 0)
    def _():
        def clear(c, carry):
            acc[c] = jnp.zeros(acc.shape[1:], acc.dtype)
            return carry
        lax.fori_loop(0, cells, clear, 0)

    for seg, vis, rows, cols in ((seg_o, vis_o, rows_o, cols_o), (seg_p, vis_p, rows_p, cols_p)):
        for i in range(batch):
            cell = seg[s * batch + i] - g * cells

            @pl.when((cell >= 0) & (cell < cells))
            def _():
                block = rows[i].reshape(span, rows.shape[-1])
                weighted = jnp.concatenate([block * vis[i, 0:1, :], block * vis[i, 1:2, :]], axis=0)
                patch = jnp.dot(weighted, cols[i], preferred_element_type=jnp.float32)
                acc[cell, :, 0:QW] += patch[:span]
                acc[cell, :, QW:2 * QW] += patch[span:]

    @pl.when(s == pl.num_programs(1) - 1)
    def _():
        def put(c, carry):
            for x in range(fold):
                out[x, c] = acc[c, x * share:(x + 1) * share, :].astype(out.dtype)
            return carry
        lax.fori_loop(0, cells, put, 0)


def patches(planes, tiles, seg_o, seg_p, half, vis_o, rows_o, cols_o, vis_p, rows_p, cols_p):
    count, fold, _, share, width = rows_o.shape
    together = 4 if planes % 4 == 0 else 1
    cells = together * tiles
    batch = 4 if count % 4 == 0 else 1
    wide = cols_o.shape[2]
    vis_spec = pl.BlockSpec((batch, 2, width), lambda g, s, a, b, h: (s, 0, 0))
    cols_spec = pl.BlockSpec((batch, width, wide), lambda g, s, a, b, h: (s, 0, 0))
    rows_own = pl.BlockSpec((batch, fold, None, share, width), lambda g, s, a, b, h: (s, 0, h[0], 0, 0))
    rows_got = pl.BlockSpec((batch, fold, share, width), lambda g, s, a, b, h: (s, 0, 0, 0))
    return pl.pallas_call(
        functools.partial(patch_kernel, cells, batch),
        out_shape=jax.ShapeDtypeStruct((fold, planes * tiles, share, 2 * wide), jnp.bfloat16),
        grid_spec=pltpu.PrefetchScalarGridSpec(
            num_scalar_prefetch=3,
            grid=(planes // together, count // batch),
            in_specs=[vis_spec, rows_own, cols_spec, vis_spec, rows_got, cols_spec],
            out_specs=pl.BlockSpec((fold, cells, share, 2 * wide), lambda g, s, a, b, h: (0, g, 0, 0)),
            scratch_shapes=[pltpu.VMEM((cells, fold * share, 2 * wide), jnp.float32)],
        ),
        compiler_params=pltpu.CompilerParams(
            dimension_semantics=("arbitrary", "arbitrary"), vmem_limit_bytes=LIMIT
        ),
        name="patches",
    )(seg_o, seg_p, half, vis_o, rows_o, cols_o, vis_p, rows_p, cols_p)


def reduce_kernel(planes, fold, turns, part, kern, out, own, xgot, zgot, lsem, xsend, xrecv, zsend, zrecv):
    me, mine = lax.axis_index("chan"), lax.axis_index("tm")
    core, row = me % 2, me // 2
    size = own.shape[1] // turns

    def x_peer(d):
        return {"chan": ((row + d) % fold) * 2 + core}

    def z_peer(d):
        return {"tm": (mine + d) % planes}

    barrier = pltpu.get_barrier_semaphore()
    for d in range(1, fold):
        pl.semaphore_signal(barrier, inc=1, device_id=x_peer(d), device_id_type=MESH)

    def hail(d, carry):
        pl.semaphore_signal(barrier, inc=1, device_id=z_peer(d), device_id_type=MESH)
        return carry
    lax.fori_loop(1, planes, hail, 0)
    pl.semaphore_wait(barrier, fold + planes - 2)

    def x_copy(j, d):
        cut = pl.ds(j * size, size)
        return pltpu.make_async_remote_copy(
            src_ref=part.at[(row + d) % fold, :, cut], dst_ref=xgot.at[d - 1, :, cut],
            send_sem=xsend.at[j, d - 1], recv_sem=xrecv.at[j, d - 1],
            device_id=x_peer(d), device_id_type=MESH,
        )

    def z_copy(j, d):
        cut = pl.ds(j * size, size)
        return pltpu.make_async_remote_copy(
            src_ref=own.at[(mine + d) % planes, cut], dst_ref=zgot.at[d - 1, cut],
            send_sem=zsend.at[j, d - 1], recv_sem=zrecv.at[j, d - 1],
            device_id=z_peer(d), device_id_type=MESH,
        )

    def l_copy(j):
        cut = pl.ds(j * size, size)
        return pltpu.make_async_copy(part.at[row, :, cut], own.at[:, cut], lsem.at[j])

    for j in range(turns):
        for d in range(1, fold):
            x_copy(j, d).start()
        l_copy(j).start()

    def over_x(w, t):
        total = own[w, t].astype(jnp.float32)
        for d in range(1, fold):
            total = total + xgot[d - 1, w, t].astype(jnp.float32)
        return total

    for j in range(turns):
        l_copy(j).wait()
        for d in range(1, fold):
            x_copy(j, d).wait_recv()

        def forward(d, carry):
            w = (mine + d) % planes
            for t in range(j * size, (j + 1) * size):
                own[w, t] = over_x(w, t).astype(own.dtype)
            z_copy(j, d).start()
            return carry
        lax.fori_loop(1, planes, forward, 0)

    share, wide = own.shape[2], own.shape[3]
    for j in range(turns):
        def arrive(d, carry):
            z_copy(j, d).wait_recv()
            return carry
        lax.fori_loop(1, planes, arrive, 0)
        for t in range(j * size, (j + 1) * size):
            def add(d, total):
                return total + zgot[d - 1, t].astype(jnp.float32)
            total = lax.fori_loop(1, planes, add, over_x(mine, t), unroll=planes <= 4)
            out[t] = jnp.dot(total.astype(jnp.bfloat16), kern[...], preferred_element_type=jnp.float32)

    for j in range(turns):
        for d in range(1, fold):
            x_copy(j, d).wait_send()

        def leave(d, carry):
            z_copy(j, d).wait_send()
            return carry
        lax.fori_loop(1, planes, leave, 0)


def reduce_grids(part, kern, planes, turns):
    fold, _, tiles, share, wide = part.shape
    return pl.pallas_call(
        functools.partial(reduce_kernel, planes, fold, turns),
        out_shape=jax.ShapeDtypeStruct((tiles, share, wide), jnp.float32),
        in_specs=[pl.BlockSpec(memory_space=pl.ANY), pl.BlockSpec(memory_space=pltpu.VMEM)],
        out_specs=pl.BlockSpec(memory_space=pltpu.VMEM),
        scratch_shapes=[
            pltpu.VMEM((planes, tiles, share, wide), jnp.bfloat16),
            pltpu.VMEM((fold - 1, planes, tiles, share, wide), jnp.bfloat16),
            pltpu.VMEM((planes - 1, tiles, share, wide), jnp.bfloat16),
            pltpu.SemaphoreType.DMA((turns,)),
            pltpu.SemaphoreType.DMA((turns, fold - 1)),
            pltpu.SemaphoreType.DMA((turns, fold - 1)),
            pltpu.SemaphoreType.DMA((turns, planes - 1)),
            pltpu.SemaphoreType.DMA((turns, planes - 1)),
        ],
        compiler_params=pltpu.CompilerParams(
            collective_id=1, has_side_effects=True, vmem_limit_bytes=LIMIT
        ),
        name="reduce_grids",
    )(part, kern)


def body(vis, row_weight, col_weight, w_bin, tile_col, w_kernel):
    planes = lax.axis_size("tm")
    chans = lax.axis_size("chan")
    count, rows_k, width_v = row_weight.shape[1:]
    tile_count = GC // QW
    share = rows_k // chans
    fold = chans // 2
    seg = w_bin[0, :, 0] * tile_count + tile_col[0]
    held = jnp.zeros((8, 128), jnp.int32).at[0, :count].set(seg)
    rows = row_weight[0].reshape(count, fold, 2, share, width_v)
    vis_p, rows_p, cols_p, held_p = swap(vis[0], rows, col_weight[0], held)
    half = (lax.axis_index("chan") % 2).reshape(1).astype(jnp.int32)
    part = patches(
        planes, tile_count, seg, held_p[0, :count], half,
        vis[0], rows, col_weight[0], vis_p, rows_p, cols_p,
    )
    part = part.reshape(fold, planes, tile_count, share, part.shape[-1])
    result = reduce_grids(part, w_kernel[0], planes, 4)
    return jnp.transpose(result, (1, 0, 2))[None]


def solution(mesh):
    in_specs = (
        P(("groups", "chan"), "tm", None, None),
        P(("groups", "chan"), "tm", None, None),
        P(("groups", "chan"), "tm", None, None),
        P(("groups", "chan"), "tm", None),
        P(("groups", "chan"), "tm"),
        P(("groups", "tm"), None, None),
    )
    out_specs = P(("groups", "tm"), "chan", None, None)
    return jax.shard_map(body, mesh=mesh, in_specs=in_specs, out_specs=out_specs, check_vma=False)
```

```python
import functools
import jax
import jax.numpy as jnp
from jax import lax
from jax.experimental import pallas as pl
from jax.experimental.pallas import tpu as pltpu
from jax.sharding import PartitionSpec as P

QW = 256
GC = 4096
MESH = pl.DeviceIdType.MESH
LIMIT = 63 * 1024 * 1024
TURNS = 8


def pair_of(me):
    return me + 1 - 2 * (me % 2)


def exchange_kernel(
    planes, tiles, turns, table, vis, rows, cols, kern, out,
    tab_s, tab_v, vis_v, rows_v, cols_v, kern_v, runs, xout, xgot, zgot,
    lsem, ssend, srecv, xsend, xrecv, zsend, zrecv,
):
    me, mine = lax.axis_index("chan"), lax.axis_index("tm")
    core, row = me % 2, me // 2
    other = pair_of(me)
    count, fold, share = rows_v.shape[1], rows_v.shape[2], rows_v.shape[3]
    size = tiles // turns

    def x_peer(d):
        return {"chan": ((row + d) % fold) * 2 + core}

    def z_peer(d):
        return {"tm": (mine + d) % planes}

    local = [
        pltpu.make_async_copy(src, dst, lsem.at[i])
        for i, (src, dst) in enumerate((
            (table, tab_s.at[0]), (vis, vis_v.at[0]), (rows.at[:, :, core], rows_v.at[0]),
            (cols, cols_v.at[0]), (kern, kern_v),
        ))
    ]
    for copy in local:
        copy.start()

    barrier = pltpu.get_barrier_semaphore()
    pl.semaphore_signal(barrier, inc=1, device_id={"chan": other}, device_id_type=MESH)
    for d in range(1, fold):
        pl.semaphore_signal(barrier, inc=1, device_id=x_peer(d), device_id_type=MESH)

    def hail(d, carry):
        pl.semaphore_signal(barrier, inc=1, device_id=z_peer(d), device_id_type=MESH)
        return carry
    lax.fori_loop(1, planes, hail, 0)
    pl.semaphore_wait(barrier, fold + planes - 1)

    swaps = [
        pltpu.make_async_remote_copy(
            src_ref=src, dst_ref=dst, send_sem=ssend.at[i], recv_sem=srecv.at[i],
            device_id={"chan": other}, device_id_type=MESH,
        )
        for i, (src, dst) in enumerate((
            (table, tab_v), (vis, vis_v.at[1]), (rows.at[:, :, other % 2], rows_v.at[1]),
            (cols, cols_v.at[1]),
        ))
    ]
    for copy in swaps:
        copy.start()

    for s in range(2):
        runs[s, 0] = jnp.zeros(runs.shape[2:], runs.dtype)

    def entry(s, i):
        return tab_s[s, i // 128, i % 128]

    batch = 4 if count % 4 == 0 else 1

    def build(s, x):
        def step(i, carry):
            found = []
            for u in range(batch):
                b = i * batch + u
                block = rows_v[s, b, x]
                weighted = jnp.concatenate(
                    [block * vis_v[s, b, 0:1, :], block * vis_v[s, b, 1:2, :]], axis=0
                )
                found.append(jnp.dot(weighted, cols_v[s, b], preferred_element_type=jnp.float32))
            for u in range(batch):
                b = i * batch + u
                last = entry(s, b)
                runs[s, b + 1, :, 0:QW] = found[u][:share] + runs[s, last, :, 0:QW]
                runs[s, b + 1, :, QW:2 * QW] = found[u][share:] + runs[s, last, :, QW:2 * QW]
            return carry
        lax.fori_loop(0, count // batch, step, 0)

    def cell(w, t):
        i = count + w * tiles + t
        return runs[0, entry(0, i)] + runs[1, entry(1, i)]

    def x_copy(j, d):
        cut = pl.ds(j * size, size)
        return pltpu.make_async_remote_copy(
            src_ref=xout.at[d - 1, :, cut], dst_ref=xgot.at[d - 1, :, cut],
            send_sem=xsend.at[j, d - 1], recv_sem=xrecv.at[j, d - 1],
            device_id=x_peer(d), device_id_type=MESH,
        )

    def z_copy(j, d):
        cut = pl.ds(j * size, size)
        return pltpu.make_async_remote_copy(
            src_ref=xgot.at[0, (mine + d) % planes, cut], dst_ref=zgot.at[d - 1, cut],
            send_sem=zsend.at[j, d - 1], recv_sem=zrecv.at[j, d - 1],
            device_id=z_peer(d), device_id_type=MESH,
        )

    for copy in local[:4]:
        copy.wait()
    for d in range(1, fold):
        half = (row + d) % fold
        build(0, half)
        if d == 1:
            for copy in swaps:
                copy.wait_recv()
            last_copy = pltpu.make_async_copy(tab_v, tab_s.at[1], lsem.at[5])
            last_copy.start()
            last_copy.wait()
        build(1, half)
        for j in range(turns):
            def fill(w, carry):
                for t in range(j * size, (j + 1) * size):
                    xout[d - 1, w, t] = cell(w, t).astype(xout.dtype)
                return carry
            lax.fori_loop(0, planes, fill, 0)
            x_copy(j, d).start()
    build(0, row)
    build(1, row)

    def over_x(w, t):
        total = cell(w, t)
        for d in range(1, fold):
            total = total + xgot[d - 1, w, t].astype(jnp.float32)
        return total

    def finish(j):
        def arrive(d, carry):
            z_copy(j, d).wait_recv()
            return carry
        lax.fori_loop(1, planes, arrive, 0)
        for t in range(j * size, (j + 1) * size):
            def add(d, total):
                return total + zgot[d - 1, t].astype(jnp.float32)
            total = lax.fori_loop(1, planes, add, over_x(mine, t), unroll=planes <= 4)
            out[t] = jnp.dot(total.astype(jnp.bfloat16), kern_v[...], preferred_element_type=jnp.float32)

    local[4].wait()
    for j in range(turns):
        for d in range(1, fold):
            x_copy(j, d).wait_recv()

        def forward(d, carry):
            w = (mine + d) % planes
            for t in range(j * size, (j + 1) * size):
                xgot[0, w, t] = over_x(w, t).astype(xgot.dtype)
            z_copy(j, d).start()
            return carry
        lax.fori_loop(1, planes, forward, 0)

    for j in range(turns):
        finish(j)

    for copy in swaps:
        copy.wait_send()
    for j in range(turns):
        for d in range(1, fold):
            x_copy(j, d).wait_send()

        def leave(d, carry):
            z_copy(j, d).wait_send()
            return carry
        lax.fori_loop(1, planes, leave, 0)


def exchange(table, vis, rows, cols, kern, planes, tiles, turns):
    count, fold, _, share, width = rows.shape
    wide = 2 * cols.shape[2]
    any_spec = pl.BlockSpec(memory_space=pl.ANY)
    half = jnp.bfloat16
    dma = pltpu.SemaphoreType.DMA
    return pl.pallas_call(
        functools.partial(exchange_kernel, planes, tiles, turns),
        out_shape=jax.ShapeDtypeStruct((tiles, share, wide), jnp.float32),
        in_specs=[any_spec] * 5,
        out_specs=pl.BlockSpec(memory_space=pltpu.VMEM),
        scratch_shapes=[
            pltpu.SMEM((2,) + table.shape, jnp.int32),
            pltpu.VMEM(table.shape, jnp.int32),
            pltpu.VMEM((2,) + vis.shape, vis.dtype),
            pltpu.VMEM((2, count, fold, share, width), rows.dtype),
            pltpu.VMEM((2,) + cols.shape, cols.dtype),
            pltpu.VMEM(kern.shape, kern.dtype),
            pltpu.VMEM((2, count + 1, share, wide), jnp.float32),
            pltpu.VMEM((fold - 1, planes, tiles, share, wide), half),
            pltpu.VMEM((fold - 1, planes, tiles, share, wide), half),
            pltpu.VMEM((planes - 1, tiles, share, wide), half),
            dma((6,)),
            dma((4,)),
            dma((4,)),
            dma((turns, fold - 1)),
            dma((turns, fold - 1)),
            dma((turns, planes - 1)),
            dma((turns, planes - 1)),
        ],
        compiler_params=pltpu.CompilerParams(
            collective_id=0, has_side_effects=True, vmem_limit_bytes=LIMIT
        ),
        name="exchange",
    )(table, vis, rows, cols, kern)


def links(seg, cells):
    count = seg.shape[0]
    place = jnp.arange(count, dtype=jnp.int32)
    same = (seg[:, None] == seg[None, :]) & (place[None, :] < place[:, None])
    before = jnp.max(jnp.where(same, place[None, :] + 1, 0), axis=1)
    named = seg[None, :] == jnp.arange(cells, dtype=jnp.int32)[:, None]
    final = jnp.max(jnp.where(named, place[None, :] + 1, 0), axis=1)
    both = jnp.concatenate([before, final])
    return jnp.pad(both, (0, -both.shape[0] % 1024)).reshape(-1, 128)


def body(vis, row_weight, col_weight, w_bin, tile_col, w_kernel):
    planes = lax.axis_size("tm")
    chans = lax.axis_size("chan")
    count, rows_k, width_v = row_weight.shape[1:]
    tile_count = GC // QW
    fold = chans // 2
    table = links(w_bin[0, :, 0] * tile_count + tile_col[0], planes * tile_count)
    rows = row_weight[0].reshape(count, fold, 2, rows_k // chans, width_v)
    result = exchange(table, vis[0], rows, col_weight[0], w_kernel[0], planes, tile_count, TURNS)
    return jnp.transpose(result, (1, 0, 2))[None]


def solution(mesh):
    in_specs = (
        P(("groups", "chan"), "tm", None, None),
        P(("groups", "chan"), "tm", None, None),
        P(("groups", "chan"), "tm", None, None),
        P(("groups", "chan"), "tm", None),
        P(("groups", "chan"), "tm"),
        P(("groups", "tm"), None, None),
    )
    out_specs = P(("groups", "tm"), "chan", None, None)
    return jax.shard_map(body, mesh=mesh, in_specs=in_specs, out_specs=out_specs, check_vma=False)
```
